32 devices in a mesh: dp: 4 (over z), win: 2 (over y), mp: 4 (over x, core).
Axes of the slice: x: 2, y: 2, z: 4, core: 2. Of those that a mesh axis runs over, the one named last changes fastest.
Arguments:
- tokens: bfloat16 [9408, 768], P(('dp', 'win', 'mp')), may hold values from -6 to 6
- target: bfloat16 [9408, 768], P(('dp', 'win', 'mp')), may hold values from -16 to 16
- regions: int32 [192, 49], P(('dp', 'win')), may hold values from 0 to 3
- rel_index: int32 [49, 49], replicated, may hold values from 0 to 168
- layer_norm_gain: float32 [768], replicated, may hold values from 0.5 to 1.5
- bias_table: float32 [169, 24], P(None, 'mp'), may hold values from -5 to 330
- w_qkv: bfloat16 [3, 768, 768], P(None, 'mp'), may hold values from -0.21875 to 0.21875
- w_proj: bfloat16 [768, 768], P('mp'), may hold values from -0.21875 to 0.21875
Outputs:
- input_gradient: float32 [9408, 768], P(('dp', 'win', 'mp'))
- grad_qkv: float32 [3, 768, 768], P(None, 'mp', ('dp', 'win'))
- grad_proj: float32 [768, 768], P('mp', ('dp', 'win'))
- grad_table: float32 [169, 24], P(None, 'mp')
- gain_gradient: float32 [768], replicated
- loss: float32 [], replicated
The draws below stay inside these ranges and needn't reach their ends.
All inputs are finite; a program needn't handle non-finite values.
Results may differ from the reference program's by a relative error of at most 0.01.
Values may be sent and summed in bfloat16 or wider, within the bound.
A program may use at most 64 MiB of HBM per device.

```python
import jax
import jax.numpy as jnp
from jax import lax

C = 768
HEADS = 24
HD = 32
WIN_TOK = 49
TABLE = 169
WINDOWS = 192
TOKENS = 9408
N_MP = 4


def draw_bias_table(key, part):
    base_key = jax.random.fold_in(jax.random.fold_in(key, 7), 0)
    base = jnp.clip(jax.random.normal(base_key, (TABLE, HEADS), jnp.float32), -5.0, 5.0)
    return base


def draw_target(key, part):
    noise_key = jax.random.fold_in(key, 11)
    fraction = jnp.arange(TOKENS, dtype=jnp.float32)[:, None] / (TOKENS - 1.0)
    noise = jnp.clip(jax.random.normal(noise_key, (TOKENS, C), jnp.float32), -4.0, 4.0)
    result = noise * (1.0 + 3.0 * fraction)
    return result.astype(jnp.bfloat16)


def touch_ends(values, rng, smallest, largest):
    place = [jax.random.randint(jax.random.fold_in(rng, axis), (), 0, length) for axis, length in enumerate(values.shape)]
    main_axis = values.shape.index(max(values.shape))
    next_to = place[:main_axis] + [(place[main_axis] + 1) % values.shape[main_axis]] + place[main_axis + 1:]
    return values.at[tuple(place)].set(smallest).at[tuple(next_to)].set(largest)


def level_of(own_key, extent, pieces, low, high):
    gain = 1.0
    for position, shards_of in pieces:
        draws = jax.random.uniform(jax.random.fold_in(jax.random.fold_in(own_key, 6), position), (shards_of,), jnp.float32, low / len(pieces), high / len(pieces))
        gain = gain * jnp.repeat(jnp.exp(draws), extent[position] // shards_of).reshape((-1,) + (1,) * (len(extent) - 1 - position))
    return gain


def centred(stream_key, shape, width, most, pieces=(), kind=jnp.bfloat16):
    entries = width * jax.random.normal(stream_key, shape, jnp.float32)
    if pieces:
        entries = entries * level_of(stream_key, shape, pieces, -0.22, 0.18)
    return jnp.clip(entries, -most, most).astype(kind)


def setup_inputs(seed: int = 0) -> dict:
    key_of = jax.random.split(jax.random.key(seed), 9)
    tokens = centred(key_of[0], (TOKENS, C), 1.0, 6.0, ((0, 32),))
    target = draw_target(jax.random.fold_in(key_of[8], 71), 0)
    regions = touch_ends(jax.random.randint(key_of[2], (WINDOWS, WIN_TOK), 0, 4), jax.random.fold_in(key_of[2], 1), 0, 3).astype(jnp.int32)
    rel_index = touch_ends(jax.random.randint(key_of[3], (WIN_TOK, WIN_TOK), 0, TABLE), jax.random.fold_in(key_of[3], 1), 0, TABLE - 1).astype(jnp.int32)
    layer_norm_gain = jnp.clip(1.0 + 0.1 * jax.random.normal(key_of[4], (C,), jnp.float32), 0.5, 1.5)
    bias_table = draw_bias_table(jax.random.fold_in(key_of[8], 71), 0)
    w_qkv = centred(key_of[6], (3, C, C), C ** -0.5, 0.21875, ((1, 4),))
    w_proj = centred(key_of[7], (C, C), C ** -0.5, 0.21875, ((0, 4),))
    return dict(tokens=tokens, target=target, regions=regions, rel_index=rel_index, layer_norm_gain=layer_norm_gain, bias_table=bias_table, w_qkv=w_qkv, w_proj=w_proj)


def group_sum(left, right, form):

    def step(total, pair):
        term = jnp.einsum(form, pair[0].astype(jnp.float32), pair[1].astype(jnp.float32))
        rounded = lax.optimization_barrier(term.astype(jnp.bfloat16))
        return (total + rounded.astype(jnp.float32), None)
    first = jnp.einsum(form, left[0].astype(jnp.float32), right[0].astype(jnp.float32))
    total, unused = lax.scan(step, jnp.zeros(first.shape, jnp.float32), (left, right))
    return total

def reference(tokens, target, regions, rel_index, layer_norm_gain, bias_table, w_qkv, w_proj):
    f32 = jnp.float32
    brain_float_sixteen = jnp.bfloat16
    group_cols = C // N_MP
    x = tokens.astype(f32)
    mean_value = lax.optimization_barrier(jnp.mean(x, axis=1, keepdims=True))
    centered_input = x - mean_value
    var = lax.optimization_barrier(jnp.mean(centered_input * centered_input, axis=1, keepdims=True))
    inverse_deviation = lax.rsqrt(var + 1e-05)
    normalized_input = centered_input * inverse_deviation
    normed_input = (normalized_input * layer_norm_gain[None, :]).astype(brain_float_sixteen)
    qkv = jnp.einsum('rc,thc->trh', normed_input.astype(f32), w_qkv.astype(f32))
    scale = HD ** (-0.5)
    shape4 = (WINDOWS, WIN_TOK, HEADS, HD)
    query = (qkv[0] * scale).astype(brain_float_sixteen).reshape(shape4)
    keys = qkv[1].astype(brain_float_sixteen).reshape(shape4)
    values = qkv[2].astype(brain_float_sixteen).reshape(shape4)
    onehot = (rel_index.reshape(-1)[:, None] == jnp.arange(TABLE, dtype=jnp.int32)[None, :]).astype(f32)
    relbias = jnp.dot(onehot, bias_table, precision=lax.Precision.HIGHEST).T.reshape(HEADS, WIN_TOK, WIN_TOK)
    maskv = jnp.where(regions[:, :, None] == regions[:, None, :], 0.0, -100.0).astype(f32)
    scores = jnp.einsum('wqhd,wkhd->whqk', query.astype(f32), keys.astype(f32))
    scores = scores + relbias[None] + maskv[:, None]
    top = lax.optimization_barrier(jnp.max(scores, axis=-1, keepdims=True))
    expo = jnp.exp(scores - top)
    probs = expo / lax.optimization_barrier(jnp.sum(expo, axis=-1, keepdims=True))
    pb = probs.astype(brain_float_sixteen)
    attn = jnp.einsum('whqk,wkhd->wqhd', pb.astype(f32), values.astype(f32)).astype(brain_float_sixteen).reshape(TOKENS, C)
    attn_groups = attn.reshape(TOKENS, N_MP, group_cols).transpose(1, 0, 2)
    proj_groups = w_proj.reshape(N_MP, group_cols, C)
    ysum = group_sum(attn_groups, proj_groups, 'rh,hc->rc')
    error_values = x + ysum - target.astype(f32)
    loss = 0.5 * jnp.sum(error_values * error_values) / TOKENS
    gb = error_values.astype(brain_float_sixteen)
    dproj = jnp.dot(attn.T, gb, preferred_element_type=f32)
    dattn = jnp.dot(gb, w_proj.T, preferred_element_type=f32).astype(brain_float_sixteen).reshape(shape4)
    dprob = jnp.einsum('wqhd,wkhd->whqk', dattn.astype(f32), values.astype(f32))
    dvalue = jnp.einsum('whqk,wqhd->wkhd', pb.astype(f32), dattn.astype(f32))
    dscore = probs * (dprob - lax.optimization_barrier(jnp.sum(probs * dprob, axis=-1, keepdims=True)))
    dtable = jnp.dot(lax.optimization_barrier(jnp.sum(dscore, axis=0)).reshape(HEADS, -1), onehot, precision=lax.Precision.HIGHEST).T
    dbf = dscore.astype(brain_float_sixteen).astype(f32)
    dquery = jnp.einsum('whqk,wkhd->wqhd', dbf, keys.astype(f32)) * scale
    dkey = jnp.einsum('whqk,wqhd->wkhd', dbf, query.astype(f32))
    dqkv = jnp.stack([dquery, dkey, dvalue]).astype(brain_float_sixteen).reshape(3, TOKENS, C)
    dwqkv = jnp.einsum('trh,rc->thc', dqkv.astype(f32), normed_input.astype(f32))
    dqkv_groups = dqkv.reshape(3, TOKENS, N_MP, group_cols).transpose(2, 0, 1, 3)
    wqkv_groups = w_qkv.reshape(3, N_MP, group_cols, C).transpose(1, 0, 2, 3)
    normed_output_gradient = group_sum(dqkv_groups, wqkv_groups, 'trh,thc->rc')
    normalized_gradient = normed_output_gradient * layer_norm_gain[None, :]
    gradient_mean_first = lax.optimization_barrier(jnp.mean(normalized_gradient, axis=1, keepdims=True))
    gradient_mean_second = lax.optimization_barrier(jnp.mean(normalized_gradient * normalized_input, axis=1, keepdims=True))
    input_gradient = error_values + inverse_deviation * (normalized_gradient - gradient_mean_first - normalized_input * gradient_mean_second)
    shrink_factor = TOKENS ** (-0.5)
    gain_gradient = lax.optimization_barrier(jnp.sum(normed_output_gradient * normalized_input, axis=0)) * shrink_factor
    return (input_gradient, dwqkv * shrink_factor, dproj * shrink_factor, dtable * shrink_factor, gain_gradient, loss)
```

```python
import functools

import jax
import jax.numpy as jnp
from jax import lax
from jax.experimental import pallas as pl
from jax.experimental.pallas import tpu as pltpu
from jax.sharding import PartitionSpec as P

HD = 32
WIN_TOK = 49
TABLE = 169
PAD = 64
LANES = 128
PACK = LANES // HD
MESH = pl.DeviceIdType.MESH
f32 = jnp.float32
bf16 = jnp.bfloat16
VM = pl.BlockSpec(memory_space=pltpu.VMEM)
NEG = -1e30


def greet(n_mp, n_win, n_dp):
    mp, win, dp = lax.axis_index("mp"), lax.axis_index("win"), lax.axis_index("dp")
    sem = pltpu.get_barrier_semaphore()
    peers = [{"mp": mp + 1 - 2 * lax.rem(mp, 2)}]
    peers += [{"mp": lax.rem(mp + 2 * d, n_mp)} for d in range(1, n_mp // 2)]
    peers += [{"win": lax.rem(win + d, n_win)} for d in range(1, n_win)]
    peers += [{"dp": lax.rem(dp + d, n_dp)} for d in range(1, n_dp)]
    for peer in peers:
        pl.semaphore_signal(sem, inc=1, device_id=peer, device_id_type=MESH)
    pl.semaphore_wait(sem, len(peers))


def sharing(hc, n_win):
    return max(n for n in range(1, n_win + 1) if n_win % n == 0 and hc % (16 * n) == 0)


def gather_kernel(n_mp, n_win, n_dp, wqkv, wproj, table, out, tab, send, recv, lsem):
    mp, win = lax.axis_index("mp"), lax.axis_index("win")
    hc = wproj.shape[0]
    share = sharing(hc, n_win)
    part = hc // share
    mine = lax.rem(win, share)
    n_x = n_mp // 2
    partner = mp + 1 - 2 * lax.rem(mp, 2)
    greet(n_mp, n_win, n_dp)

    def block(group):
        return out.at[:, pl.ds(pl.multiple_of(group * hc, 16), hc), :]

    def piece(group, p):
        return out.at[:, pl.ds(pl.multiple_of(group * hc + p * part, 16), part), :]

    own = [
        pltpu.make_async_copy(wqkv, out.at[pl.ds(0, 3), pl.ds(pl.multiple_of(mp * hc, 16), hc), :], lsem.at[0]),
        pltpu.make_async_copy(wproj, out.at[3, pl.ds(pl.multiple_of(mp * hc, 16), hc), :], lsem.at[1]),
        pltpu.make_async_copy(table, tab.at[mp], lsem.at[2]),
    ]
    for c in own:
        c.start()
    for c in own:
        c.wait()
    started = []
    count = [0]

    def start(src, dst, peer):
        c = pltpu.make_async_remote_copy(
            src_ref=src, dst_ref=dst, send_sem=send.at[count[0]], recv_sem=recv.at[count[0]],
            device_id=peer, device_id_type=MESH,
        )
        count[0] += 1
        c.start()
        started.append(c)
        return c

    across, tabs = [], []
    for d in range(1, n_x):
        peer = {"mp": lax.rem(mp + 2 * d, n_mp)}
        tabs.append(start(tab.at[mp], tab.at[mp], peer))
        across.append(start(piece(mp, mine), piece(mp, mine), peer))
    beside = [start(block(mp), block(mp), {"mp": partner}),
              start(tab.at[mp], tab.at[mp], {"mp": partner})]
    later = []
    for d in range(1, n_x):
        group = lax.rem(mp - 2 * d + n_mp, n_mp)
        tabs[d - 1].wait_recv()
        across[d - 1].wait_recv()
        here = []
        for e in range(1, share):
            other = win - mine + lax.rem(mine + e, share)
            here.append(start(piece(group, mine), piece(group, mine), {"win": other}))
        beside.append(start(piece(group, mine), piece(group, mine), {"mp": partner}))
        beside.append(start(tab.at[group], tab.at[group], {"mp": partner}))
        later.append((group, here))
    for group, here in later:
        for e in range(1, share):
            here[e - 1].wait_recv()
            p = lax.rem(mine - e + share, share)
            beside.append(start(piece(group, p), piece(group, p), {"mp": partner}))
    for c in beside:
        c.wait_recv()
    for c in started:
        c.wait_send()


def dot(a, b, ca, cb):
    return lax.dot_general(a, b, (((ca,), (cb,)), ((), ())), preferred_element_type=f32)


def layer_kernel(n_mp, x_ref, t_ref, gain_ref, w_ref, bias_ref, mask_ref,
                 ig_ref, g_ref, ds_ref, gg_ref, loss_ref,
                 xhat, inv, xn, qs, ks, vs, probs, at, gb, da, dq, dk, dv, dxn):
    R, C = x_ref.shape
    W = R // PAD
    ng = C // LANES
    scale = HD ** (-0.5)
    gain = gain_ref[...]
    lane_head = lax.broadcasted_iota(jnp.int32, (PAD, LANES), 1) // HD

    def rows_of(w):
        return pl.ds(pl.multiple_of(w * PAD, PAD), PAD)

    @pl.loop(0, W)
    def _(w):
        r = rows_of(w)
        xf = x_ref[r, :].astype(f32)
        cen = xf - jnp.mean(xf, axis=1, keepdims=True)
        iv = lax.rsqrt(jnp.mean(cen * cen, axis=1, keepdims=True) + 1e-05)
        xh = cen * iv
        xhat[r, :] = xh
        inv[r, :] = jnp.broadcast_to(iv, (PAD, LANES))
        xn[r, :] = (xh * gain).astype(bf16)

    BN = 256
    for t, (dst, sc) in enumerate(((qs, scale), (ks, None), (vs, None))):
        @pl.loop(0, C // BN)
        def _(j, t=t, dst=dst, sc=sc):
            c = pl.ds(pl.multiple_of(j * BN, BN), BN)
            y = dot(xn[...], w_ref[t, c, :], 1, 1)
            if sc is not None:
                y = y * sc
            dst[:, c] = y.astype(bf16)

    def spread(a):
        zero = jnp.zeros_like(a)
        return jnp.concatenate([jnp.where(lane_head == h, a, zero) for h in range(PACK)], axis=0)

    def fold(a):
        total = jnp.zeros((PAD, LANES), f32)
        for h in range(PACK):
            total = jnp.where(lane_head == h, a[h * PAD:(h + 1) * PAD], total)
        return total

    @pl.loop(0, ng)
    def _(g):
        c = pl.ds(pl.multiple_of(g * LANES, LANES), LANES)
        for w in range(W):
            r = pl.ds(w * PAD, PAD)
            s = dot(spread(ks[r, c]), qs[r, c], 1, 1)
            s = s.reshape(PACK, PAD, PAD) + bias_ref[g] + mask_ref[w][None]
            e = jnp.exp(s - jnp.max(s, axis=1, keepdims=True))
            p = e / jnp.sum(e, axis=1, keepdims=True)
            p = p.reshape(PACK * PAD, PAD)
            probs[g * W + w] = p
            at[r, c] = dot(p.astype(bf16), spread(vs[r, c]), 0, 0).astype(bf16)

    loss_ref[...] = jnp.zeros_like(loss_ref)
    @pl.loop(0, C // BN)
    def _(j):
        c = pl.ds(pl.multiple_of(j * BN, BN), BN)
        y = dot(at[...], w_ref[3, :, c], 1, 0)
        e = x_ref[:, c].astype(f32) + y - t_ref[:, c].astype(f32)
        row = lax.broadcasted_iota(jnp.int32, e.shape, 0) % PAD
        e = jnp.where(row < WIN_TOK, e, 0.0)
        ig_ref[:, c] = e
        gb[:, c] = e.astype(bf16)
        loss_ref[...] += jnp.sum(e * e, axis=0, keepdims=True)

    @pl.loop(0, C // BN)
    def _(j):
        c = pl.ds(pl.multiple_of(j * BN, BN), BN)
        da[:, c] = dot(gb[...], w_ref[3, c, :], 1, 1).astype(bf16)

    @pl.loop(0, ng)
    def _(g):
        c = pl.ds(pl.multiple_of(g * LANES, LANES), LANES)
        total = jnp.zeros((PACK * PAD, PAD), f32)
        for w in range(W):
            r = pl.ds(w * PAD, PAD)
            p = probs[g * W + w]
            do = da[r, c]
            dp = dot(spread(vs[r, c]), do, 1, 1)
            pd = (p * dp).reshape(PACK, PAD, PAD)
            ds = p.reshape(PACK, PAD, PAD) * (
                dp.reshape(PACK, PAD, PAD) - jnp.sum(pd, axis=1, keepdims=True))
            ds = ds.reshape(PACK * PAD, PAD)
            total = total + ds
            db = ds.astype(bf16)
            dv[r, c] = fold(dot(p.astype(bf16), do, 1, 0)).astype(bf16)
            dk[r, c] = fold(dot(db, qs[r, c], 1, 0)).astype(bf16)
            dq[r, c] = (dot(db, spread(ks[r, c]), 0, 0) * scale).astype(bf16)
        ds_ref[g] = total

    @pl.loop(0, C // BN)
    def _(j):
        c = pl.ds(pl.multiple_of(j * BN, BN), BN)
        y = dot(dq[...], w_ref[0, :, c], 1, 0)
        y += dot(dk[...], w_ref[1, :, c], 1, 0)
        y += dot(dv[...], w_ref[2, :, c], 1, 0)
        dxn[:, c] = y

    gg_ref[...] = jnp.zeros_like(gg_ref)

    @pl.loop(0, W)
    def _(w):
        r = rows_of(w)
        d, xh = dxn[r, :], xhat[r, :]
        gg_ref[...] += jnp.sum(d * xh, axis=0, keepdims=True)
        dh = d * gain
        m1 = jnp.mean(dh, axis=1, keepdims=True)
        m2 = jnp.mean(dh * xh, axis=1, keepdims=True)
        ig_ref[r, :] += inv[r, 0:1] * (dh - m1 - xh * m2)

    hc = C // n_mp
    xnt = xn[...].T
    gbt = gb[...].T
    for m in range(n_mp):
        lo = m * hc
        d = jnp.concatenate([a[:, lo:lo + hc] for a in (dq, dk, dv)], axis=1)
        g_ref[m] = jnp.concatenate(
            [dot(xnt, d, 1, 0).astype(bf16), dot(gbt, at[:, lo:lo + hc], 1, 0).astype(bf16)], axis=1)


def reduce_kernel(n_mp, n_win, n_dp, g_ref, small_ref, out_ref, tot_ref,
                  r_core, h, ra, rb, a1, b1, ra2, rb2, a2, rz, s_core, s1, sx, s2, sw, s3, sz,
                  send, recv):
    n_x = n_mp // 2
    mp, win, dp = lax.axis_index("mp"), lax.axis_index("win"), lax.axis_index("dp")
    core, x = lax.rem(mp, 2), mp // 2
    half = n_dp // 2
    greet(n_mp, n_win, n_dp)
    started = []

    def start(src, dst, peer):
        i = len(started)
        c = pltpu.make_async_remote_copy(
            src_ref=src, dst_ref=dst, send_sem=send.at[i], recv_sem=recv.at[i],
            device_id=peer, device_id_type=MESH,
        )
        c.start()
        started.append(c)
        return c

    def add(*terms):
        total = terms[0].astype(f32)
        for t in terms[1:]:
            total = total + t.astype(f32)
        return total

    def on_x(d):
        return {"mp": lax.rem(mp + 2 * d, n_mp)}, lax.rem(x + d, n_x)

    def on_win(d):
        return {"win": lax.rem(win + d, n_win)}, lax.rem(win + d, n_win)

    def on_dp(d):
        return {"dp": lax.rem(dp + d, n_dp)}, lax.rem(dp + d, n_dp)

    partner = {"mp": mp + 1 - 2 * core}
    c0 = start(small_ref, s_core, partner)
    firsts = [start(g_ref.at[i, 1 - core], r_core.at[i], partner) for i in range(n_x)]
    c0.wait_recv()
    s1[...] = small_ref[...] + s_core[...]

    def exchange_small(src, slots, on, n, own):
        cs = [start(src, slots.at[own], on(d)[0]) for d in range(1, n)]
        return cs

    def finish_small(cs, src, slots, own, n, dst):
        slots[own] = src[...]
        for c in cs:
            c.wait_recv()
        total = slots[0]
        for i in range(1, n):
            total = total + slots[i]
        dst[...] = total

    cx = exchange_small(s1, sx, on_x, n_x, x)
    for i in range(n_x):
        firsts[i].wait_recv()
        h[i] = add(g_ref[i, core], r_core[i]).astype(bf16)
    ca = [start(h.at[on_x(d)[1], :, pl.ds(0, half)], ra.at[d - 1], on_x(d)[0]) for d in range(1, n_x)]
    cb = [start(h.at[:, on_win(d)[1], pl.ds(half, half)], rb.at[d - 1], on_win(d)[0])
          for d in range(1, n_win)]
    finish_small(cx, s1, sx, x, n_x, s2)
    cw = exchange_small(s2, sw, on_win, n_win, win)
    for c in ca:
        c.wait_recv()
    a1[...] = add(h[x, :, 0:half], *[ra[d] for d in range(n_x - 1)]).astype(bf16)
    ca = [start(a1.at[on_win(d)[1]], ra2.at[d - 1], on_win(d)[0]) for d in range(1, n_win)]
    for c in cb:
        c.wait_recv()
    b1[...] = add(h[:, win, half:2 * half], *[rb[d] for d in range(n_win - 1)]).astype(bf16)
    cb = [start(b1.at[on_x(d)[1]], rb2.at[d - 1], on_x(d)[0]) for d in range(1, n_x)]
    finish_small(cw, s2, sw, win, n_win, s3)
    cz = exchange_small(s3, sz, on_dp, n_dp, dp)
    for c in ca:
        c.wait_recv()
    a2[0:half] = add(a1[win], *[ra2[d] for d in range(n_win - 1)]).astype(bf16)
    for c in cb:
        c.wait_recv()
    a2[half:2 * half] = add(b1[x], *[rb2[d] for d in range(n_x - 1)]).astype(bf16)
    zs = [start(a2.at[on_dp(d)[1]], rz.at[d - 1], on_dp(d)[0]) for d in range(1, n_dp)]
    finish_small(cz, s3, sz, dp, n_dp, tot_ref)
    for c in zs:
        c.wait_recv()
    out_ref[...] = add(a2[dp], *[rz[d] for d in range(n_dp - 1)])
    for c in started:
        c.wait_send()


def per_device(sizes, tokens, target, regions, rel_index, gain, bias_table, w_qkv, w_proj):
    n_dp, n_win, n_mp = sizes
    n_x = n_mp // 2
    rows, C = tokens.shape
    W = rows // WIN_TOK
    hc = w_proj.shape[0]
    nh = hc // HD
    heads = nh * n_mp
    R = W * PAD
    ng = C // LANES
    everyone = rows * n_dp * n_win * n_mp
    SDS = jax.ShapeDtypeStruct
    big = 60 * 1024 * 1024

    copies = 2 * (n_x - 1) + 2 + (n_x - 1) * (2 * (sharing(hc, n_win) - 1) + 2)
    table = jnp.pad(bias_table.T, ((0, 8 - nh), (0, 2 * LANES - TABLE)))
    weights, tables = pl.pallas_call(
        functools.partial(gather_kernel, n_mp, n_win, n_dp),
        out_shape=(SDS((4, C, C), bf16), SDS((n_mp, 8, 2 * LANES), f32)),
        in_specs=[VM] * 3, out_specs=(VM, VM),
        scratch_shapes=[pltpu.SemaphoreType.DMA((copies,)), pltpu.SemaphoreType.DMA((copies,)),
                        pltpu.SemaphoreType.DMA((3,))],
        compiler_params=pltpu.CompilerParams(collective_id=0, has_side_effects=True),
        name="gather",
    )(w_qkv, w_proj, table)

    index = jnp.pad(rel_index.T, ((0, PAD - WIN_TOK), (0, PAD - WIN_TOK)), constant_values=-1)
    onehot = (index.reshape(-1)[None, :] == jnp.arange(2 * LANES, dtype=jnp.int32)[:, None]).astype(f32)
    full = tables[:, :nh].reshape(heads, 2 * LANES)
    bias = jnp.dot(full, onehot, precision=lax.Precision.HIGHEST).reshape(ng, PACK, PAD, PAD)
    key_pad = jnp.where(jnp.arange(PAD) < WIN_TOK, 0.0, NEG)[:, None]
    bias = bias + key_pad
    mine = lax.dynamic_slice_in_dim(regions, lax.axis_index("mp") * W, W, 0)
    mine = jnp.pad(mine, ((0, 0), (0, PAD - WIN_TOK)))
    maskv = jnp.where(mine[:, :, None] == mine[:, None, :], 0.0, -100.0).astype(f32)

    def padded(a):
        a = a.reshape(W, WIN_TOK, C)
        return jnp.pad(a, ((0, 0), (0, PAD - WIN_TOK), (0, 0))).reshape(R, C)

    act = pltpu.VMEM((R, C), bf16)
    wide = pltpu.VMEM((R, C), f32)
    ig, grads, ds, gg, loss = pl.pallas_call(
        functools.partial(layer_kernel, n_mp),
        out_shape=(SDS((R, C), f32), SDS((n_mp, C, 4 * hc), bf16), SDS((ng, PACK * PAD, PAD), f32),
                   SDS((1, C), f32), SDS((1, 256), f32)),
        in_specs=[VM] * 6, out_specs=(VM,) * 5,
        scratch_shapes=[wide, pltpu.VMEM((R, LANES), f32), act, act, act, act,
                        pltpu.VMEM((ng * W, PACK * PAD, PAD), f32),
                        act, act, act, act, act, act, wide],
        compiler_params=pltpu.CompilerParams(vmem_limit_bytes=big),
        name="layer",
    )(padded(tokens), padded(target), gain[None, :], weights, bias, maskv)

    dtab = jnp.dot(ds.reshape(heads, PAD * PAD), onehot.T, precision=lax.Precision.HIGHEST)
    extra = jnp.concatenate([gg.reshape(C // 256, 256), loss], axis=0)
    small = jnp.concatenate([dtab, extra], axis=0)
    small = jnp.pad(small, ((0, -small.shape[0] % 8), (0, 0)))
    cpd = C // (n_dp * n_win)
    L = 4 * hc
    half = n_dp // 2
    grads = grads.reshape(n_x, 2, n_dp, n_win, cpd, L).transpose(0, 1, 3, 2, 4, 5)
    sm = small.shape
    copies = 1 + n_x + 3 * (n_x - 1) + 3 * (n_win - 1) + 2 * (n_dp - 1)
    V = pltpu.VMEM
    out, tot = pl.pallas_call(
        functools.partial(reduce_kernel, n_mp, n_win, n_dp),
        out_shape=(SDS((cpd, L), f32), SDS(sm, f32)),
        in_specs=[VM] * 2, out_specs=(VM, VM),
        scratch_shapes=[
            V((n_x, n_win, n_dp, cpd, L), bf16),
            V((n_x, n_win, n_dp, cpd, L), bf16),
            V((max(n_x - 1, 1), n_win, half, cpd, L), bf16),
            V((max(n_win - 1, 1), n_x, half, cpd, L), bf16),
            V((n_win, half, cpd, L), bf16),
            V((n_x, half, cpd, L), bf16),
            V((max(n_win - 1, 1), half, cpd, L), bf16),
            V((max(n_x - 1, 1), half, cpd, L), bf16),
            V((n_dp, cpd, L), bf16),
            V((n_dp - 1, cpd, L), bf16),
            V(sm, f32), V(sm, f32), V((n_x,) + sm, f32), V(sm, f32), V((n_win,) + sm, f32),
            V(sm, f32), V((n_dp,) + sm, f32),
            pltpu.SemaphoreType.DMA((copies,)), pltpu.SemaphoreType.DMA((copies,)),
        ],
        compiler_params=pltpu.CompilerParams(
            collective_id=1, has_side_effects=True, vmem_limit_bytes=big),
        name="reduce",
    )(grads, small)

    s = everyone ** (-0.5)
    out = (out * s).reshape(cpd, 4, hc).transpose(1, 2, 0)
    tot_heads = lax.dynamic_slice_in_dim(tot[:heads, :TABLE], lax.axis_index("mp") * nh, nh, 0)
    gain_gradient = tot[heads:heads + C // 256].reshape(C) * s
    loss = 0.5 * jnp.sum(tot[heads + C // 256]) / everyone
    return (ig.reshape(W, PAD, C)[:, :WIN_TOK].reshape(rows, C), out[:3], out[3],
            tot_heads.T * s, gain_gradient, loss)


def solution(mesh):
    sizes = (mesh.shape["dp"], mesh.shape["win"], mesh.shape["mp"])
    in_specs = (
        P(("dp", "win", "mp"), None),
        P(("dp", "win", "mp"), None),
        P(("dp", "win"), None),
        P(),
        P(),
        P(None, "mp"),
        P(None, "mp", None),
        P("mp", None),
    )
    out_specs = (
        P(("dp", "win", "mp"), None),
        P(None, "mp", ("dp", "win")),
        P("mp", ("dp", "win")),
        P(None, "mp"),
        P(),
        P(),
    )
    return jax.shard_map(
        functools.partial(per_device, sizes), mesh=mesh, in_specs=in_specs, out_specs=out_specs,
        check_vma=False,
    )
```

```python
import functools

import jax
import jax.numpy as jnp
from jax import lax
from jax.experimental import pallas as pl
from jax.experimental.pallas import tpu as pltpu
from jax.sharding import PartitionSpec as P

HD = 32
WIN_TOK = 49
TABLE = 169
PAD = 64
LANES = 128
PACK = LANES // HD
MESH = pl.DeviceIdType.MESH
f32 = jnp.float32
bf16 = jnp.bfloat16
VM = pl.BlockSpec(memory_space=pltpu.VMEM)
NEG = -1e30


def greet(n_mp, n_win, n_dp):
    mp, win, dp = lax.axis_index("mp"), lax.axis_index("win"), lax.axis_index("dp")
    sem = pltpu.get_barrier_semaphore()
    peers = [{"mp": mp + 1 - 2 * lax.rem(mp, 2)}]
    peers += [{"mp": lax.rem(mp + 2 * d, n_mp)} for d in range(1, n_mp // 2)]
    peers += [{"win": lax.rem(win + d, n_win)} for d in range(1, n_win)]
    peers += [{"dp": lax.rem(dp + d, n_dp)} for d in range(1, n_dp)]
    for peer in peers:
        pl.semaphore_signal(sem, inc=1, device_id=peer, device_id_type=MESH)
    pl.semaphore_wait(sem, len(peers))


def sharing(hc, n_win):
    return max(n for n in range(1, n_win + 1) if n_win % n == 0 and hc % (16 * n) == 0)


def dot(a, b, ca, cb):
    return lax.dot_general(a, b, (((ca,), (cb,)), ((), ())), preferred_element_type=f32)


class Link:
    def __init__(self, send, recv):
        self.send, self.recv, self.started = send, recv, []

    def __call__(self, src, dst, peer):
        i = len(self.started)
        c = pltpu.make_async_remote_copy(
            src_ref=src, dst_ref=dst, send_sem=self.send.at[i], recv_sem=self.recv.at[i],
            device_id=peer, device_id_type=MESH,
        )
        c.start()
        self.started.append(c)
        return c


def add(*terms):
    total = terms[0].astype(f32)
    for t in terms[1:]:
        total = total + t.astype(f32)
    return total


def layer_kernel(n_mp, n_win, n_dp, everyone,
                 x_ref, t_ref, gain_ref, wqkv, wproj, table, index_ref, mask_ref,
                 ig_ref, out_ref, tot_ref,
                 w_ref, tab, bias, xt, xhat, inv, xn, qs, ks, vs, probs, at, gb, da, dq, dk, dv, dxn,
                 ds_ref, gg, sq, small,
                 g_ref, r_core, h, ra, rb, a1, b1, ra2, rb2, a2, rz,
                 s_core, s1, sx, s2, sw, s3, sz, send, recv, lsem):
    mp, win, dp = lax.axis_index("mp"), lax.axis_index("win"), lax.axis_index("dp")
    core, x = lax.rem(mp, 2), mp // 2
    R, C = xhat.shape
    W = R // PAD
    ng = C // LANES
    hc = C // n_mp
    nh = hc // HD
    n_x = n_mp // 2
    cpd = C // (n_dp * n_win)
    half = n_dp // 2
    share = sharing(hc, n_win)
    part = hc // share
    mine = lax.rem(win, share)
    scale = HD ** (-0.5)
    partner = {"mp": mp + 1 - 2 * core}
    start = Link(send, recv)
    BN = 256

    def across(group, size=hc, off=0):
        return pl.ds(pl.multiple_of(group * hc + off, 16), size)

    def own(t, rows):
        return wqkv.at[t, rows, :] if t < 3 else wproj.at[rows, :]

    local = [pltpu.make_async_copy(own(t, pl.ds(0, hc)), w_ref.at[t, across(mp), :], lsem.at[t])
             for t in range(4)]
    local.append(pltpu.make_async_copy(table, tab.at[mp], lsem.at[4]))
    for c in local:
        c.start()
    greet(n_mp, n_win, n_dp)
    tabx = [start(table, tab.at[mp], {"mp": lax.rem(mp + 2 * d, n_mp)}) for d in range(1, n_x)]
    tabs = [start(table, tab.at[mp], partner)]
    first, ready = [], []
    for t in range(4):
        first.append([])
        for d in range(1, n_x):
            first[t].append(start(
                own(t, pl.ds(pl.multiple_of(mine * part, 16), part)),
                w_ref.at[t, across(mp, part, mine * part), :], {"mp": lax.rem(mp + 2 * d, n_mp)}))
    for t in range(4):
        ready.append([start(own(t, pl.ds(0, hc)), w_ref.at[t, across(mp), :], partner)])

    second = [[] for _ in range(4)]

    def pass_on(t):
        for d in range(1, n_x):
            group = lax.rem(mp - 2 * d + n_mp, n_mp)
            ref = w_ref.at[t, across(group, part, mine * part), :]
            first[t][d - 1].wait_recv()
            for e in range(1, share):
                other = win - mine + lax.rem(mine + e, share)
                second[t].append((group, e, start(ref, ref, {"win": other})))
            ready[t].append(start(ref, ref, partner))

    def pass_rest(t):
        for group, e, c in second[t]:
            c.wait_recv()
            p = lax.rem(mine - e + share, share)
            ref = w_ref.at[t, across(group, part, p * part), :]
            ready[t].append(start(ref, ref, partner))

    def complete(t):
        for c in ready[t]:
            c.wait_recv()

    gain = gain_ref[...]
    lane_head = lax.broadcasted_iota(jnp.int32, (PAD, LANES), 1) // HD
    blank = jnp.zeros((PAD - WIN_TOK, C), f32)
    for w in range(W):
        r = pl.ds(w * PAD, PAD)
        src = pl.ds(w * WIN_TOK, WIN_TOK)
        xf = jnp.concatenate([x_ref[src, :].astype(f32), blank], axis=0)
        tf = jnp.concatenate([t_ref[src, :].astype(f32), blank], axis=0)
        xt[r, :] = xf - tf
        cen = xf - jnp.mean(xf, axis=1, keepdims=True)
        iv = lax.rsqrt(jnp.mean(cen * cen, axis=1, keepdims=True) + 1e-05)
        xh = cen * iv
        xhat[r, :] = xh
        inv[r, :] = jnp.broadcast_to(iv, (PAD, LANES))
        xn[r, :] = (xh * gain).astype(bf16)
    for d in range(1, n_x):
        group = lax.rem(mp - 2 * d + n_mp, n_mp)
        tabx[d - 1].wait_recv()
        tabs.append(start(tab.at[group], tab.at[group], partner))
    for c in local:
        c.wait()
    for c in tabs:
        c.wait_recv()
    pass_on(0)

    entries = lax.broadcasted_iota(jnp.int32, (2 * LANES, PAD), 0)

    def thirds(a):
        hi = a.astype(bf16)
        rest = a - hi.astype(f32)
        mid = rest.astype(bf16)
        low = (rest - mid.astype(f32)).astype(bf16)
        return jnp.concatenate([hi, mid, low], axis=0)

    tabn = 8 * n_mp
    table3 = thirds(tab[...].reshape(tabn, 2 * LANES))

    def fill_bias(lo, hi):
        @pl.loop(lo // 8, hi // 8)
        def _(kk):
            for u in range(8):
                k = kk * 8 + u
                onehot = (entries == index_ref[pl.ds(k, 1), :]).astype(f32).astype(bf16)
                b = dot(table3, onehot, 1, 0)
                b = b[:tabn] + b[tabn:2 * tabn] + b[2 * tabn:]
                b = b + jnp.where(k < WIN_TOK, 0.0, NEG)
                for head in range(n_mp * nh):
                    row = head // nh * 8 + head % nh
                    bias[head // PACK, pl.ds(head % PACK * PAD + k, 1), :] = b[row:row + 1]

    fill_bias(0, PAD // 2)
    pass_on(1)
    fill_bias(PAD // 2, PAD)

    def project(t, dst, sc):
        @pl.loop(0, C // BN)
        def _(j):
            c = pl.ds(pl.multiple_of(j * BN, BN), BN)
            y = dot(xn[...], w_ref[t, c, :], 1, 1)
            if sc is not None:
                y = y * sc
            dst[:, c] = y.astype(bf16)

    pass_rest(0)
    pass_on(2)
    complete(0)
    project(0, qs, scale)
    pass_rest(1)
    pass_on(3)
    complete(1)
    project(1, ks, None)
    pass_rest(2)
    complete(2)
    project(2, vs, None)

    def spread(a):
        zero = jnp.zeros_like(a)
        return jnp.concatenate([jnp.where(lane_head == i, a, zero) for i in range(PACK)], axis=0)

    def fold(a):
        total = jnp.zeros((PAD, LANES), f32)
        for i in range(PACK):
            total = jnp.where(lane_head == i, a[i * PAD:(i + 1) * PAD], total)
        return total

    def forward(lo, hi):
        @pl.loop(lo, hi)
        def _(g):
            c = pl.ds(pl.multiple_of(g * LANES, LANES), LANES)
            for w in range(W):
                r = pl.ds(w * PAD, PAD)
                s = dot(spread(ks[r, c]), qs[r, c], 1, 1) + bias[g]
                s = s.reshape(PACK, PAD, PAD) + mask_ref[w][None]
                e = jnp.exp(s - jnp.max(s, axis=1, keepdims=True))
                p = e / jnp.sum(e, axis=1, keepdims=True)
                p = p.reshape(PACK * PAD, PAD)
                probs[g * W + w] = p
                at[r, c] = dot(p.astype(bf16), spread(vs[r, c]), 0, 0).astype(bf16)

    forward(0, ng // 3)
    pass_rest(3)
    forward(ng // 3, ng)
    complete(3)

    sq[...] = jnp.zeros_like(sq)

    @pl.loop(0, C // BN)
    def _(j):
        c = pl.ds(pl.multiple_of(j * BN, BN), BN)
        e = xt[:, c] + dot(at[...], w_ref[3, :, c], 1, 0)
        row = lax.broadcasted_iota(jnp.int32, e.shape, 0) % PAD
        e = jnp.where(row < WIN_TOK, e, 0.0)
        xt[:, c] = e
        gb[:, c] = e.astype(bf16)
        sq[...] += jnp.sum(e * e, axis=0, keepdims=True)

    @pl.loop(0, C // BN)
    def _(j):
        c = pl.ds(pl.multiple_of(j * BN, BN), BN)
        da[:, c] = dot(gb[...], w_ref[3, c, :], 1, 1).astype(bf16)

    @pl.loop(0, ng)
    def _(g):
        c = pl.ds(pl.multiple_of(g * LANES, LANES), LANES)
        total = jnp.zeros((PACK * PAD, PAD), f32)
        for w in range(W):
            r = pl.ds(w * PAD, PAD)
            p = probs[g * W + w]
            do = da[r, c]
            dprob = dot(spread(vs[r, c]), do, 1, 1)
            p3, d3 = p.reshape(PACK, PAD, PAD), dprob.reshape(PACK, PAD, PAD)
            ds = p3 * (d3 - jnp.sum(p3 * d3, axis=1, keepdims=True))
            ds = ds.reshape(PACK * PAD, PAD)
            total = total + ds
            db = ds.astype(bf16)
            dv[r, c] = fold(dot(p.astype(bf16), do, 1, 0)).astype(bf16)
            dk[r, c] = fold(dot(db, qs[r, c], 1, 0)).astype(bf16)
            dq[r, c] = (dot(db, spread(ks[r, c]), 0, 0) * scale).astype(bf16)
        ds_ref[g] = total

    waves = 2 if cpd % 32 == 0 else 1
    deep = cpd // waves
    xnt = xn[...].T
    gbt = gb[...].T
    firsts = []
    for i in range(n_x):
        for cc in range(2):
            lo = (2 * i + cc) * hc
            d = jnp.concatenate([a[:, lo:lo + hc] for a in (dq, dk, dv)], axis=1)
            y = jnp.concatenate(
                [dot(xnt, d, 1, 0), dot(gbt, at[:, lo:lo + hc], 1, 0)], axis=1)
            for u in range(n_dp):
                for v in range(n_win):
                    o = (u * n_win + v) * cpd
                    g_ref[i, cc, v, u] = y[o:o + cpd].astype(bf16)
        firsts.append([start(g_ref.at[i, 1 - core, :, :, pl.ds(f * deep, deep)],
                             r_core.at[i, :, :, pl.ds(f * deep, deep)], partner)
                       for f in range(waves)])

    def on_x(d):
        return {"mp": lax.rem(mp + 2 * d, n_mp)}, lax.rem(x + d, n_x)

    def on_win(d):
        return {"win": lax.rem(win + d, n_win)}, lax.rem(win + d, n_win)

    def on_dp(d):
        return {"dp": lax.rem(dp + d, n_dp)}, lax.rem(dp + d, n_dp)

    def rows(f):
        return pl.ds(f * deep, deep)

    lo_dp, hi_dp = pl.ds(0, half), pl.ds(half, half)
    stage = {}

    def step1(f):
        for i in range(n_x):
            firsts[i][f].wait_recv()
            h[i, :, :, rows(f)] = add(g_ref[i, core, :, :, rows(f)],
                                      r_core[i, :, :, rows(f)]).astype(bf16)
        ca = [start(h.at[on_x(d)[1], :, lo_dp, rows(f)], ra.at[d - 1, :, :, rows(f)], on_x(d)[0])
              for d in range(1, n_x)]
        cb = [start(h.at[:, on_win(d)[1], hi_dp, rows(f)], rb.at[d - 1, :, :, rows(f)], on_win(d)[0])
              for d in range(1, n_win)]
        stage[f] = ca, cb

    def step2(f):
        ca, cb = stage[f]
        for c in ca:
            c.wait_recv()
        a1[:, :, rows(f)] = add(h[x, :, lo_dp, rows(f)],
                                *[ra[d, :, :, rows(f)] for d in range(n_x - 1)]).astype(bf16)
        na = [start(a1.at[on_win(d)[1], :, rows(f)], ra2.at[d - 1, :, rows(f)], on_win(d)[0])
              for d in range(1, n_win)]
        for c in cb:
            c.wait_recv()
        b1[:, :, rows(f)] = add(h[:, win, hi_dp, rows(f)],
                                *[rb[d, :, :, rows(f)] for d in range(n_win - 1)]).astype(bf16)
        nb = [start(b1.at[on_x(d)[1], :, rows(f)], rb2.at[d - 1, :, rows(f)], on_x(d)[0])
              for d in range(1, n_x)]
        stage[f] = na, nb

    def step3(f):
        ca, cb = stage[f]
        for c in ca:
            c.wait_recv()
        a2[lo_dp, rows(f)] = add(a1[win, :, rows(f)],
                                 *[ra2[d, :, rows(f)] for d in range(n_win - 1)]).astype(bf16)
        for c in cb:
            c.wait_recv()
        a2[hi_dp, rows(f)] = add(b1[x, :, rows(f)],
                                 *[rb2[d, :, rows(f)] for d in range(n_x - 1)]).astype(bf16)
        stage[f] = [start(a2.at[on_dp(d)[1], rows(f)], rz.at[d - 1, rows(f)], on_dp(d)[0])
                    for d in range(1, n_dp)]

    def step4(f):
        for c in stage[f]:
            c.wait_recv()
        y = add(a2[dp, rows(f)], *[rz[d, rows(f)] for d in range(n_dp - 1)])
        out_ref[rows(f), :] = y * everyone ** (-0.5)

    for f in range(waves):
        step1(f)

    @pl.loop(0, C // BN)
    def _(j):
        c = pl.ds(pl.multiple_of(j * BN, BN), BN)
        y = dot(dq[...], w_ref[0, :, c], 1, 0)
        y += dot(dk[...], w_ref[1, :, c], 1, 0)
        y += dot(dv[...], w_ref[2, :, c], 1, 0)
        dxn[:, c] = y

    gg[...] = jnp.zeros_like(gg)

    def finish(w):
        r = pl.ds(w * PAD, PAD)
        d, xh = dxn[r, :], xhat[r, :]
        gg[...] += jnp.sum(d * xh, axis=0, keepdims=True)
        dh = d * gain
        m1 = jnp.mean(dh, axis=1, keepdims=True)
        m2 = jnp.mean(dh * xh, axis=1, keepdims=True)
        y = xt[r, :] + inv[r, 0:1] * (dh - m1 - xh * m2)
        ig_ref[pl.ds(w * WIN_TOK, WIN_TOK), :] = y[:WIN_TOK]

    for w in range(W):
        finish(w)

    step2(0)
    heads = n_mp * nh
    small[...] = jnp.zeros_like(small)
    hp = ng * PACK

    @pl.loop(0, PAD // 8)
    def _(kk):
        total = jnp.zeros((3 * hp, 2 * LANES), f32)
        for u in range(8):
            k = kk * 8 + u
            onehot = (entries == index_ref[pl.ds(k, 1), :]).astype(f32).astype(bf16)
            one = jnp.concatenate(
                [ds_ref[i // PACK, pl.ds(i % PACK * PAD + k, 1), :] for i in range(hp)], axis=0)
            total = total + dot(thirds(one), onehot, 1, 1)
        small[0:hp, :] += total[:hp] + total[hp:2 * hp] + total[2 * hp:]

    for i in range(C // BN):
        small[heads + i:heads + i + 1, :] = gg[:, i * BN:(i + 1) * BN]
    small[heads + C // BN:heads + C // BN + 1, :] = sq[...]

    cc0 = start(small, s_core, partner)
    for f in range(1, waves):
        step2(f)

    def share_small(src, slots, on, n):
        def begin(me):
            return [start(src, slots.at[me], on(d)[0]) for d in range(1, n)]
        return begin

    def finish_small(cs, src, slots, me, n, dst):
        slots[me] = src[...]
        for c in cs:
            c.wait_recv()
        total = slots[0]
        for i in range(1, n):
            total = total + slots[i]
        dst[...] = total

    cc0.wait_recv()
    s1[...] = small[...] + s_core[...]
    cx = share_small(s1, sx, on_x, n_x)(x)
    step3(0)
    finish_small(cx, s1, sx, x, n_x, s2)
    cw = share_small(s2, sw, on_win, n_win)(win)
    finish_small(cw, s2, sw, win, n_win, s3)
    cz = share_small(s3, sz, on_dp, n_dp)(dp)
    for f in range(1, waves):
        step3(f)
    finish_small(cz, s3, sz, dp, n_dp, tot_ref)
    for f in range(waves):
        step4(f)
    for c in start.started:
        c.wait_send()


def per_device(sizes, tokens, target, regions, rel_index, gain, bias_table, w_qkv, w_proj):
    n_dp, n_win, n_mp = sizes
    n_x = n_mp // 2
    rows, C = tokens.shape
    W = rows // WIN_TOK
    hc = w_proj.shape[0]
    nh = hc // HD
    heads = nh * n_mp
    R = W * PAD
    ng = C // LANES
    everyone = rows * n_dp * n_win * n_mp
    SDS = jax.ShapeDtypeStruct
    V = pltpu.VMEM

    table = jnp.pad(bias_table.T, ((0, 8 - nh), (0, 2 * LANES - TABLE)))
    index = jnp.pad(rel_index.T, ((0, PAD - WIN_TOK), (0, PAD - WIN_TOK)), constant_values=-1)
    mine = lax.dynamic_slice_in_dim(regions, lax.axis_index("mp") * W, W, 0)
    mine = jnp.pad(mine, ((0, 0), (0, PAD - WIN_TOK)))
    maskv = jnp.where(mine[:, :, None] == mine[:, None, :], 0.0, -100.0).astype(f32)

    cpd = C // (n_dp * n_win)
    L = 4 * hc
    half = n_dp // 2
    waves = 2 if cpd % 32 == 0 else 1
    share = sharing(hc, n_win)
    copies = n_x + 4 * (n_x - 1) + 4 + (n_x - 1) * (1 + 4 * (2 * (share - 1) + 1))
    copies += waves * (n_x + 2 * (n_x - 1) + 2 * (n_win - 1) + n_dp - 1)
    copies += 1 + (n_x - 1) + (n_win - 1) + (n_dp - 1)
    srows = heads + C // 256 + 1
    sm = (srows + -srows % 8, 256)
    act = V((R, C), bf16)
    wide = V((R, C), f32)
    ig, out, tot = pl.pallas_call(
        functools.partial(layer_kernel, n_mp, n_win, n_dp, everyone),
        out_shape=(SDS((rows, C), f32), SDS((cpd, L), f32), SDS(sm, f32)),
        in_specs=[VM] * 8, out_specs=(VM,) * 3,
        scratch_shapes=[
            V((4, C, C), bf16), V((n_mp, 8, 2 * LANES), f32), V((ng, PACK * PAD, PAD), f32),
            wide, wide, V((R, LANES), f32), act, act, act, act,
            V((ng * W, PACK * PAD, PAD), f32),
            act, act, act, act, act, act, wide,
            V((ng, PACK * PAD, PAD), f32), V((1, C), f32), V((1, 256), f32), V(sm, f32),
            V((n_x, 2, n_win, n_dp, cpd, L), bf16),
            V((n_x, n_win, n_dp, cpd, L), bf16),
            V((n_x, n_win, n_dp, cpd, L), bf16),
            V((max(n_x - 1, 1), n_win, half, cpd, L), bf16),
            V((max(n_win - 1, 1), n_x, half, cpd, L), bf16),
            V((n_win, half, cpd, L), bf16),
            V((n_x, half, cpd, L), bf16),
            V((max(n_win - 1, 1), half, cpd, L), bf16),
            V((max(n_x - 1, 1), half, cpd, L), bf16),
            V((n_dp, cpd, L), bf16),
            V((n_dp - 1, cpd, L), bf16),
            V(sm, f32), V(sm, f32), V((n_x,) + sm, f32), V(sm, f32), V((n_win,) + sm, f32),
            V(sm, f32), V((n_dp,) + sm, f32),
            pltpu.SemaphoreType.DMA((copies,)), pltpu.SemaphoreType.DMA((copies,)),
            pltpu.SemaphoreType.DMA((5,)),
        ],
        compiler_params=pltpu.CompilerParams(
            collective_id=0, has_side_effects=True, vmem_limit_bytes=60 * 1024 * 1024),
        name="layer",
    )(tokens, target, gain[None, :], w_qkv, w_proj, table, index, maskv)

    s = everyone ** (-0.5)
    out = out.reshape(cpd, 4, hc).transpose(1, 2, 0)
    tot_heads = lax.dynamic_slice_in_dim(tot[:heads, :TABLE], lax.axis_index("mp") * nh, nh, 0)
    gain_gradient = tot[heads:heads + C // 256].reshape(C) * s
    loss = 0.5 * jnp.sum(tot[heads + C // 256]) / everyone
    return ig, out[:3], out[3], tot_heads.T * s, gain_gradient, loss


def solution(mesh):
    sizes = (mesh.shape["dp"], mesh.shape["win"], mesh.shape["mp"])
    in_specs = (
        P(("dp", "win", "mp"), None),
        P(("dp", "win", "mp"), None),
        P(("dp", "win"), None),
        P(),
        P(),
        P(None, "mp"),
        P(None, "mp", None),
        P("mp", None),
    )
    out_specs = (
        P(("dp", "win", "mp"), None),
        P(None, "mp", ("dp", "win")),
        P("mp", ("dp", "win")),
        P(None, "mp"),
        P(),
        P(),
    )
    return jax.shard_map(
        functools.partial(per_device, sizes), mesh=mesh, in_specs=in_specs, out_specs=out_specs,
        check_vma=False,
    )
```

```python
import functools

import jax
import jax.numpy as jnp
from jax import lax
from jax.experimental import pallas as pl
from jax.experimental.pallas import tpu as pltpu
from jax.sharding import PartitionSpec as P

HD = 32
WIN_TOK = 49
TABLE = 169
PAD = 64
LANES = 128
PACK = LANES // HD
MESH = pl.DeviceIdType.MESH
f32 = jnp.float32
bf16 = jnp.bfloat16
VM = pl.BlockSpec(memory_space=pltpu.VMEM)
NEG = -1e30


def greet(n_mp, n_win, n_dp):
    mp, win, dp = lax.axis_index("mp"), lax.axis_index("win"), lax.axis_index("dp")
    sem = pltpu.get_barrier_semaphore()
    peers = [{"mp": mp + 1 - 2 * lax.rem(mp, 2)}]
    peers += [{"mp": lax.rem(mp + 2 * d, n_mp)} for d in range(1, n_mp // 2)]
    peers += [{"win": lax.rem(win + d, n_win)} for d in range(1, n_win)]
    peers += [{"dp": lax.rem(dp + d, n_dp)} for d in range(1, n_dp)]
    for peer in peers:
        pl.semaphore_signal(sem, inc=1, device_id=peer, device_id_type=MESH)
    pl.semaphore_wait(sem, len(peers))


def sharing(hc, n_win):
    return max(n for n in range(1, n_win + 1) if n_win % n == 0 and hc % (16 * n) == 0)


def dot(a, b, ca, cb):
    return lax.dot_general(a, b, (((ca,), (cb,)), ((), ())), preferred_element_type=f32)


class Link:
    def __init__(self, send, recv):
        self.send, self.recv, self.started = send, recv, []

    def __call__(self, src, dst, peer):
        i = len(self.started)
        c = pltpu.make_async_remote_copy(
            src_ref=src, dst_ref=dst, send_sem=self.send.at[i], recv_sem=self.recv.at[i],
            device_id=peer, device_id_type=MESH,
        )
        c.start()
        self.started.append(c)
        return c


def add(*terms):
    total = terms[0].astype(f32)
    for t in terms[1:]:
        total = total + t.astype(f32)
    return total


def layer_kernel(n_mp, n_win, n_dp, everyone,
                 x_ref, t_ref, gain_ref, wqkv, wproj, table, index_ref, mask_ref,
                 ig_ref, out_ref, tot_ref,
                 w_ref, tab, bias, xt, xhat, inv, xn, qs, ks, vs, probs, at, gb, da, dq, dk, dv, dxn,
                 ds_ref, gg, sq, small,
                 g_ref, r_core, h, ra, rb, a1, b1, ra2, rb2, a2, rz,
                 s_core, s1, sx, s2, sw, s3, sz, send, recv, lsem):
    mp, win, dp = lax.axis_index("mp"), lax.axis_index("win"), lax.axis_index("dp")
    core, x = lax.rem(mp, 2), mp // 2
    R, C = xhat.shape
    W = R // PAD
    ng = C // LANES
    hc = C // n_mp
    nh = hc // HD
    n_x = n_mp // 2
    cpd = C // (n_dp * n_win)
    half = n_dp // 2
    share = sharing(hc, n_win)
    part = hc // share
    mine = lax.rem(win, share)
    scale = HD ** (-0.5)
    partner = {"mp": mp + 1 - 2 * core}
    start = Link(send, recv)
    BN = 256

    def across(group, size=hc, off=0):
        return pl.ds(pl.multiple_of(group * hc + off, 16), size)

    def own(t, rows):
        return wqkv.at[t, rows, :] if t < 3 else wproj.at[rows, :]

    local = [pltpu.make_async_copy(own(t, pl.ds(0, hc)), w_ref.at[t, across(mp), :], lsem.at[t])
             for t in range(4)]
    local.append(pltpu.make_async_copy(table, tab.at[mp], lsem.at[4]))
    for c in local:
        c.start()
    greet(n_mp, n_win, n_dp)
    tabx = [start(table, tab.at[mp], {"mp": lax.rem(mp + 2 * d, n_mp)}) for d in range(1, n_x)]
    tabs = [start(table, tab.at[mp], partner)]
    first, ready = [], []
    for t in range(4):
        first.append([])
        for d in range(1, n_x):
            first[t].append(start(
                own(t, pl.ds(pl.multiple_of(mine * part, 16), part)),
                w_ref.at[t, across(mp, part, mine * part), :], {"mp": lax.rem(mp + 2 * d, n_mp)}))
    for t in range(4):
        ready.append([start(own(t, pl.ds(0, hc)), w_ref.at[t, across(mp), :], partner)])

    second = [[] for _ in range(4)]

    def pass_on(t):
        for d in range(1, n_x):
            group = lax.rem(mp - 2 * d + n_mp, n_mp)
            ref = w_ref.at[t, across(group, part, mine * part), :]
            first[t][d - 1].wait_recv()
            for e in range(1, share):
                other = win - mine + lax.rem(mine + e, share)
                second[t].append((group, e, start(ref, ref, {"win": other})))
            ready[t].append(start(ref, ref, partner))

    def pass_rest(t):
        for group, e, c in second[t]:
            c.wait_recv()
            p = lax.rem(mine - e + share, share)
            ref = w_ref.at[t, across(group, part, p * part), :]
            ready[t].append(start(ref, ref, partner))

    def complete(t):
        for c in ready[t]:
            c.wait_recv()

    gain = gain_ref[...]
    lane_head = lax.broadcasted_iota(jnp.int32, (PAD, LANES), 1) // HD
    blank = jnp.zeros((PAD - WIN_TOK, C), f32)
    for w in range(W):
        r = pl.ds(w * PAD, PAD)
        src = pl.ds(w * WIN_TOK, WIN_TOK)
        xf = jnp.concatenate([x_ref[src, :].astype(f32), blank], axis=0)
        tf = jnp.concatenate([t_ref[src, :].astype(f32), blank], axis=0)
        xt[r, :] = xf - tf
        cen = xf - jnp.mean(xf, axis=1, keepdims=True)
        iv = lax.rsqrt(jnp.mean(cen * cen, axis=1, keepdims=True) + 1e-05)
        xh = cen * iv
        xhat[r, :] = xh
        inv[r, :] = jnp.broadcast_to(iv, (PAD, LANES))
        xn[r, :] = (xh * gain).astype(bf16)
    for d in range(1, n_x):
        group = lax.rem(mp - 2 * d + n_mp, n_mp)
        tabx[d - 1].wait_recv()
        tabs.append(start(tab.at[group], tab.at[group], partner))
    for c in local:
        c.wait()
    for c in tabs:
        c.wait_recv()
    pass_on(0)

    entries = lax.broadcasted_iota(jnp.int32, (2 * LANES, PAD), 0)

    def thirds(a):
        hi = a.astype(bf16)
        rest = a - hi.astype(f32)
        mid = rest.astype(bf16)
        low = (rest - mid.astype(f32)).astype(bf16)
        return jnp.concatenate([hi, mid, low], axis=0)

    tabn = 8 * n_mp
    table3 = thirds(tab[...].reshape(tabn, 2 * LANES))

    def fill_bias(lo, hi):
        @pl.loop(lo // 8, hi // 8)
        def _(kk):
            for u in range(8):
                k = kk * 8 + u
                onehot = (entries == index_ref[pl.ds(k, 1), :]).astype(f32).astype(bf16)
                b = dot(table3, onehot, 1, 0)
                b = b[:tabn] + b[tabn:2 * tabn] + b[2 * tabn:]
                b = b + jnp.where(k < WIN_TOK, 0.0, NEG)
                for head in range(n_mp * nh):
                    row = head // nh * 8 + head % nh
                    bias[head // PACK, pl.ds(head % PACK * PAD + k, 1), :] = b[row:row + 1]

    fill_bias(0, PAD // 2)
    pass_on(1)
    fill_bias(PAD // 2, PAD)

    def project(t, dst, sc):
        @pl.loop(0, C // BN)
        def _(j):
            c = pl.ds(pl.multiple_of(j * BN, BN), BN)
            y = dot(xn[...], w_ref[t, c, :], 1, 1)
            if sc is not None:
                y = y * sc
            dst[:, c] = y.astype(bf16)

    pass_rest(0)
    pass_on(2)
    complete(0)
    project(0, qs, scale)
    pass_rest(1)
    pass_on(3)
    complete(1)
    project(1, ks, None)
    pass_rest(2)
    complete(2)
    project(2, vs, None)

    def spread(a):
        zero = jnp.zeros_like(a)
        return jnp.concatenate([jnp.where(lane_head == i, a, zero) for i in range(PACK)], axis=0)

    def fold(a):
        total = jnp.zeros((PAD, LANES), f32)
        for i in range(PACK):
            total = jnp.where(lane_head == i, a[i * PAD:(i + 1) * PAD], total)
        return total

    def forward(lo, hi):
        @pl.loop(lo, hi)
        def _(g):
            c = pl.ds(pl.multiple_of(g * LANES, LANES), LANES)
            for w in range(W):
                r = pl.ds(w * PAD, PAD)
                s = dot(spread(ks[r, c]), qs[r, c], 1, 1) + bias[g]
                s = s.reshape(PACK, PAD, PAD) + mask_ref[w][None]
                e = jnp.exp(s - jnp.max(s, axis=1, keepdims=True))
                p = e / jnp.sum(e, axis=1, keepdims=True)
                p = p.reshape(PACK * PAD, PAD)
                probs[g * W + w] = p
                at[r, c] = dot(p.astype(bf16), spread(vs[r, c]), 0, 0).astype(bf16)

    forward(0, ng // 3)
    pass_rest(3)
    forward(ng // 3, ng)
    complete(3)

    sq[...] = jnp.zeros_like(sq)

    @pl.loop(0, C // BN)
    def _(j):
        c = pl.ds(pl.multiple_of(j * BN, BN), BN)
        e = xt[:, c] + dot(at[...], w_ref[3, :, c], 1, 0)
        row = lax.broadcasted_iota(jnp.int32, e.shape, 0) % PAD
        e = jnp.where(row < WIN_TOK, e, 0.0)
        xt[:, c] = e
        gb[:, c] = e.astype(bf16)
        sq[...] += jnp.sum(e * e, axis=0, keepdims=True)

    @pl.loop(0, C // BN)
    def _(j):
        c = pl.ds(pl.multiple_of(j * BN, BN), BN)
        da[:, c] = dot(gb[...], w_ref[3, c, :], 1, 1).astype(bf16)

    @pl.loop(0, ng)
    def _(g):
        c = pl.ds(pl.multiple_of(g * LANES, LANES), LANES)
        total = jnp.zeros((PACK * PAD, PAD), f32)
        for w in range(W):
            r = pl.ds(w * PAD, PAD)
            p = probs[g * W + w]
            do = da[r, c]
            dprob = dot(spread(vs[r, c]), do, 1, 1)
            p3, d3 = p.reshape(PACK, PAD, PAD), dprob.reshape(PACK, PAD, PAD)
            ds = p3 * (d3 - jnp.sum(p3 * d3, axis=1, keepdims=True))
            ds = ds.reshape(PACK * PAD, PAD)
            total = total + ds
            db = ds.astype(bf16)
            dv[r, c] = fold(dot(p.astype(bf16), do, 1, 0)).astype(bf16)
            dk[r, c] = fold(dot(db, qs[r, c], 1, 0)).astype(bf16)
            dq[r, c] = (dot(db, spread(ks[r, c]), 0, 0) * scale).astype(bf16)
        ds_ref[g] = total

    waves = cpd // 32 if cpd % 32 == 0 else 1
    deep = cpd // waves
    xnt = xn[...].T
    gbt = gb[...].T
    firsts = []
    for i in range(n_x):
        for cc in range(2):
            lo = (2 * i + cc) * hc
            d = jnp.concatenate([a[:, lo:lo + hc] for a in (dq, dk, dv)], axis=1)
            y = jnp.concatenate(
                [dot(xnt, d, 1, 0), dot(gbt, at[:, lo:lo + hc], 1, 0)], axis=1)
            for u in range(n_dp):
                for v in range(n_win):
                    o = (u * n_win + v) * cpd
                    g_ref[i, cc, v, u] = y[o:o + cpd].astype(bf16)
        firsts.append([start(g_ref.at[i, 1 - core, :, :, pl.ds(f * deep, deep)],
                             r_core.at[i, :, :, pl.ds(f * deep, deep)], partner)
                       for f in range(waves)])

    def on_x(d):
        return {"mp": lax.rem(mp + 2 * d, n_mp)}, lax.rem(x + d, n_x)

    def on_win(d):
        return {"win": lax.rem(win + d, n_win)}, lax.rem(win + d, n_win)

    def on_dp(d):
        return {"dp": lax.rem(dp + d, n_dp)}, lax.rem(dp + d, n_dp)

    def rows(f):
        return pl.ds(f * deep, deep)

    lo_dp, hi_dp = pl.ds(0, half), pl.ds(half, half)
    stage = {}

    def step1(f):
        for i in range(n_x):
            firsts[i][f].wait_recv()
            h[i, :, :, rows(f)] = add(g_ref[i, core, :, :, rows(f)],
                                      r_core[i, :, :, rows(f)]).astype(bf16)
        ca = [start(h.at[on_x(d)[1], :, lo_dp, rows(f)], ra.at[d - 1, :, :, rows(f)], on_x(d)[0])
              for d in range(1, n_x)]
        cb = [start(h.at[:, on_win(d)[1], hi_dp, rows(f)], rb.at[d - 1, :, :, rows(f)], on_win(d)[0])
              for d in range(1, n_win)]
        stage[f] = ca, cb

    def step2(f):
        ca, cb = stage[f]
        for c in ca:
            c.wait_recv()
        a1[:, :, rows(f)] = add(h[x, :, lo_dp, rows(f)],
                                *[ra[d, :, :, rows(f)] for d in range(n_x - 1)]).astype(bf16)
        na = [start(a1.at[on_win(d)[1], :, rows(f)], ra2.at[d - 1, :, rows(f)], on_win(d)[0])
              for d in range(1, n_win)]
        for c in cb:
            c.wait_recv()
        b1[:, :, rows(f)] = add(h[:, win, hi_dp, rows(f)],
                                *[rb[d, :, :, rows(f)] for d in range(n_win - 1)]).astype(bf16)
        nb = [start(b1.at[on_x(d)[1], :, rows(f)], rb2.at[d - 1, :, rows(f)], on_x(d)[0])
              for d in range(1, n_x)]
        stage[f] = na, nb

    def step3(f):
        ca, cb = stage[f]
        for c in ca:
            c.wait_recv()
        a2[lo_dp, rows(f)] = add(a1[win, :, rows(f)],
                                 *[ra2[d, :, rows(f)] for d in range(n_win - 1)]).astype(bf16)
        for c in cb:
            c.wait_recv()
        a2[hi_dp, rows(f)] = add(b1[x, :, rows(f)],
                                 *[rb2[d, :, rows(f)] for d in range(n_x - 1)]).astype(bf16)
        stage[f] = [start(a2.at[on_dp(d)[1], rows(f)], rz.at[d - 1, rows(f)], on_dp(d)[0])
                    for d in range(1, n_dp)]

    def step4(f):
        for c in stage[f]:
            c.wait_recv()
        y = add(a2[dp, rows(f)], *[rz[d, rows(f)] for d in range(n_dp - 1)])
        out_ref[rows(f), :] = y * everyone ** (-0.5)

    for f in range(min(waves, 2)):
        step1(f)

    @pl.loop(0, C // BN)
    def _(j):
        c = pl.ds(pl.multiple_of(j * BN, BN), BN)
        y = dot(dq[...], w_ref[0, :, c], 1, 0)
        y += dot(dk[...], w_ref[1, :, c], 1, 0)
        y += dot(dv[...], w_ref[2, :, c], 1, 0)
        dxn[:, c] = y

    step2(0)
    for f in range(2, waves):
        step1(f)
    gg[...] = jnp.zeros_like(gg)

    def finish(w):
        r = pl.ds(w * PAD, PAD)
        d, xh = dxn[r, :], xhat[r, :]
        gg[...] += jnp.sum(d * xh, axis=0, keepdims=True)
        dh = d * gain
        m1 = jnp.mean(dh, axis=1, keepdims=True)
        m2 = jnp.mean(dh * xh, axis=1, keepdims=True)
        y = xt[r, :] + inv[r, 0:1] * (dh - m1 - xh * m2)
        ig_ref[pl.ds(w * WIN_TOK, WIN_TOK), :] = y[:WIN_TOK]

    for w in range(W):
        finish(w)

    if waves > 1:
        step2(1)
    heads = n_mp * nh
    small[...] = jnp.zeros_like(small)
    hp = ng * PACK

    @pl.loop(0, PAD // 8)
    def _(kk):
        total = jnp.zeros((3 * hp, 2 * LANES), f32)
        for u in range(8):
            k = kk * 8 + u
            onehot = (entries == index_ref[pl.ds(k, 1), :]).astype(f32).astype(bf16)
            one = jnp.concatenate(
                [ds_ref[i // PACK, pl.ds(i % PACK * PAD + k, 1), :] for i in range(hp)], axis=0)
            total = total + dot(thirds(one), onehot, 1, 1)
        small[0:hp, :] += total[:hp] + total[hp:2 * hp] + total[2 * hp:]

    for i in range(C // BN):
        small[heads + i:heads + i + 1, :] = gg[:, i * BN:(i + 1) * BN]
    small[heads + C // BN:heads + C // BN + 1, :] = sq[...]

    cc0 = start(small, s_core, partner)
    step3(0)
    for f in range(2, waves):
        step2(f)

    def share_small(src, slots, on, n):
        def begin(me):
            return [start(src, slots.at[me], on(d)[0]) for d in range(1, n)]
        return begin

    def finish_small(cs, src, slots, me, n, dst):
        slots[me] = src[...]
        for c in cs:
            c.wait_recv()
        total = slots[0]
        for i in range(1, n):
            total = total + slots[i]
        dst[...] = total

    cc0.wait_recv()
    s1[...] = small[...] + s_core[...]
    cx = share_small(s1, sx, on_x, n_x)(x)
    if waves > 1:
        step3(1)
    finish_small(cx, s1, sx, x, n_x, s2)
    cw = share_small(s2, sw, on_win, n_win)(win)
    for f in range(2, waves):
        step3(f)
    finish_small(cw, s2, sw, win, n_win, s3)
    cz = share_small(s3, sz, on_dp, n_dp)(dp)
    finish_small(cz, s3, sz, dp, n_dp, tot_ref)
    for f in range(waves):
        step4(f)
    for c in start.started:
        c.wait_send()


def per_device(sizes, tokens, target, regions, rel_index, gain, bias_table, w_qkv, w_proj):
    n_dp, n_win, n_mp = sizes
    n_x = n_mp // 2
    rows, C = tokens.shape
    W = rows // WIN_TOK
    hc = w_proj.shape[0]
    nh = hc // HD
    heads = nh * n_mp
    R = W * PAD
    ng = C // LANES
    everyone = rows * n_dp * n_win * n_mp
    SDS = jax.ShapeDtypeStruct
    V = pltpu.VMEM

    table = jnp.pad(bias_table.T, ((0, 8 - nh), (0, 2 * LANES - TABLE)))
    index = jnp.pad(rel_index.T, ((0, PAD - WIN_TOK), (0, PAD - WIN_TOK)), constant_values=-1)
    mine = lax.dynamic_slice_in_dim(regions, lax.axis_index("mp") * W, W, 0)
    mine = jnp.pad(mine, ((0, 0), (0, PAD - WIN_TOK)))
    maskv = jnp.where(mine[:, :, None] == mine[:, None, :], 0.0, -100.0).astype(f32)

    cpd = C // (n_dp * n_win)
    L = 4 * hc
    half = n_dp // 2
    waves = cpd // 32 if cpd % 32 == 0 else 1
    share = sharing(hc, n_win)
    copies = n_x + 4 * (n_x - 1) + 4 + (n_x - 1) * (1 + 4 * (2 * (share - 1) + 1))
    copies += waves * (n_x + 2 * (n_x - 1) + 2 * (n_win - 1) + n_dp - 1)
    copies += 1 + (n_x - 1) + (n_win - 1) + (n_dp - 1)
    srows = heads + C // 256 + 1
    sm = (srows + -srows % 8, 256)
    act = V((R, C), bf16)
    wide = V((R, C), f32)
    ig, out, tot = pl.pallas_call(
        functools.partial(layer_kernel, n_mp, n_win, n_dp, everyone),
        out_shape=(SDS((rows, C), f32), SDS((cpd, L), f32), SDS(sm, f32)),
        in_specs=[VM] * 8, out_specs=(VM,) * 3,
        scratch_shapes=[
            V((4, C, C), bf16), V((n_mp, 8, 2 * LANES), f32), V((ng, PACK * PAD, PAD), f32),
            wide, wide, V((R, LANES), f32), act, act, act, act,
            V((ng * W, PACK * PAD, PAD), f32),
            act, act, act, act, act, act, wide,
            V((ng, PACK * PAD, PAD), f32), V((1, C), f32), V((1, 256), f32), V(sm, f32),
            V((n_x, 2, n_win, n_dp, cpd, L), bf16),
            V((n_x, n_win, n_dp, cpd, L), bf16),
            V((n_x, n_win, n_dp, cpd, L), bf16),
            V((max(n_x - 1, 1), n_win, half, cpd, L), bf16),
            V((max(n_win - 1, 1), n_x, half, cpd, L), bf16),
            V((n_win, half, cpd, L), bf16),
            V((n_x, half, cpd, L), bf16),
            V((max(n_win - 1, 1), half, cpd, L), bf16),
            V((max(n_x - 1, 1), half, cpd, L), bf16),
            V((n_dp, cpd, L), bf16),
            V((n_dp - 1, cpd, L), bf16),
            V(sm, f32), V(sm, f32), V((n_x,) + sm, f32), V(sm, f32), V((n_win,) + sm, f32),
            V(sm, f32), V((n_dp,) + sm, f32),
            pltpu.SemaphoreType.DMA((copies,)), pltpu.SemaphoreType.DMA((copies,)),
            pltpu.SemaphoreType.DMA((5,)),
        ],
        compiler_params=pltpu.CompilerParams(
            collective_id=0, has_side_effects=True, vmem_limit_bytes=60 * 1024 * 1024),
        name="layer",
    )(tokens, target, gain[None, :], w_qkv, w_proj, table, index, maskv)

    s = everyone ** (-0.5)
    out = out.reshape(cpd, 4, hc).transpose(1, 2, 0)
    tot_heads = lax.dynamic_slice_in_dim(tot[:heads, :TABLE], lax.axis_index("mp") * nh, nh, 0)
    gain_gradient = tot[heads:heads + C // 256].reshape(C) * s
    loss = 0.5 * jnp.sum(tot[heads + C // 256]) / everyone
    return ig, out[:3], out[3], tot_heads.T * s, gain_gradient, loss


def solution(mesh):
    sizes = (mesh.shape["dp"], mesh.shape["win"], mesh.shape["mp"])
    in_specs = (
        P(("dp", "win", "mp"), None),
        P(("dp", "win", "mp"), None),
        P(("dp", "win"), None),
        P(),
        P(),
        P(None, "mp"),
        P(None, "mp", None),
        P("mp", None),
    )
    out_specs = (
        P(("dp", "win", "mp"), None),
        P(None, "mp", ("dp", "win")),
        P("mp", ("dp", "win")),
        P(None, "mp"),
        P(),
        P(),
    )
    return jax.shard_map(
        functools.partial(per_device, sizes), mesh=mesh, in_specs=in_specs, out_specs=out_specs,
        check_vma=False,
    )
```
